32 devices in a mesh: grp: 2 (over x), wide: 16 (over z, y, core).
Axes of the slice: x: 2, y: 2, z: 4, core: 2. Of those that a mesh axis runs over, the one named last changes fastest.
Arguments:
- x_pool: bfloat16 [16384, 7168], P(('grp', 'wide')), may hold values from -6 to 6
- token_ids: int32 [4096], P(('grp', 'wide')), may hold values from 0 to 16383, as said below
- cotangent: bfloat16 [4096, 7168], P(('grp', 'wide')), may hold values from -6 to 6
- gate_up: bfloat16 [2, 1024, 7168], P(None, 'wide', 'grp'), may hold values from -0.0625 to 0.0625
- down_weight: bfloat16 [1024, 7168], P('wide', 'grp'), may hold values from -0.1875 to 0.1875
- loss_exponent: int32 [1], replicated, may hold values from 3 to 9
Outputs:
- grad_gate_up: bfloat16 [2, 1024, 7168], P(None, 'wide', 'grp')
- grad_down: bfloat16 [1024, 7168], P('wide', 'grp')
The draws below stay inside these ranges and needn't reach their ends.
Inputs may be any that keep to these rules, and one draw needn't show every extreme that they name: The 128 ids in aligned block b of token_ids name rows b * 512 to (b + 1) * 512 - 1 of x_pool.
All inputs are finite; a program needn't handle non-finite values.
Results may differ from the reference program's by a relative error of at most 0.014.
Values may be sent and summed in bfloat16 or wider, within the bound.
A program may use at most 192 MiB of HBM per device.

```python
import jax
import jax.numpy as jnp
import numpy as np

D = 7168
F = 1024
BLOCKS = 8
TOK_DEV = 128
POOL_DEV = 512
TOKENS = 4096
POOL = 16384
N_GRP = 2
N_WIDE = 16


def draw_token_ids(key, part):
    offsets = jnp.arange(TOKENS, dtype=jnp.int32) // TOK_DEV * POOL_DEV
    return offsets + jax.random.randint(key, (TOKENS,), 0, POOL_DEV, dtype=jnp.int32)


def shard_levels(key, shape, pieces, smallest, top_value):
    level, own = 1.0, jax.random.fold_in(key, 6)
    for dim, shards_of in pieces:
        heights = jnp.exp(jax.random.uniform(jax.random.fold_in(own, dim), (shards_of,), jnp.float32, smallest / len(pieces), top_value / len(pieces)))
        level = level * jnp.repeat(heights, shape[dim] // shards_of).reshape([-1 if axis == dim else 1 for axis in range(len(shape))])
    return level


def scatter_about(key, extent, width, limit, cuts=(), held_as=jnp.bfloat16):
    gain = shard_levels(key, extent, cuts, -0.22, 0.18) if cuts else 1.0
    drawn = jax.random.normal(key, extent, jnp.float32) * width * gain
    return jnp.minimum(jnp.maximum(drawn, -limit), limit).astype(held_as)


def setup_inputs(seed: int = 0) -> dict:
    key_of = jax.random.split(jax.random.key(seed), 7)
    return {
        "x_pool": scatter_about(key_of[0], (POOL, D), 1.0, 6.0, ((0, 32),)),
        "token_ids": draw_token_ids(jax.random.fold_in(key_of[6], 71), 0),
        "cotangent": scatter_about(key_of[2], (TOKENS, D), 1.0, 6.0, ((0, 32),)),
        "gate_up": scatter_about(key_of[3], (2, F, D), D ** -0.5, 0.0625, ((1, 16), (2, 2))),
        "down_weight": scatter_about(key_of[4], (F, D), F ** -0.5, 0.1875, ((0, 16), (1, 2))),
        "loss_exponent": jax.random.randint(key_of[5], (1,), 3, 10).astype(jnp.int32),
    }


def unscale_of(loss_exponent):
    levels = jnp.arange(16, dtype=jnp.int32)
    powers = jnp.asarray(np.power(0.5, np.arange(16)), dtype=jnp.float32)
    return jnp.sum(jnp.where(levels == loss_exponent[0], powers, jnp.float32(0.0)))


def reference(x_pool, token_ids, cotangent, gate_up, down_weight, loss_exponent):
    picked = jnp.take(x_pool, token_ids, axis=0)
    unscale = unscale_of(loss_exponent)
    gate_act = jnp.dot(picked, gate_up[0].T, preferred_element_type=jnp.float32)
    up_act = jnp.dot(picked, gate_up[1].T, preferred_element_type=jnp.float32)
    delta_hidden = unscale * jnp.dot(cotangent, down_weight.T, preferred_element_type=jnp.float32)
    sigmoid_gate = jax.nn.sigmoid(gate_act)
    hidden = (gate_act * sigmoid_gate * up_act).astype(jnp.bfloat16)
    delta_gate = (delta_hidden * up_act * sigmoid_gate * (1.0 + gate_act * (1.0 - sigmoid_gate))).astype(jnp.bfloat16)
    delta_up = (delta_hidden * gate_act * sigmoid_gate).astype(jnp.bfloat16)
    set_count = N_GRP * (N_WIDE // BLOCKS)
    set_rows = TOKENS // set_count
    total_gate = jnp.zeros((F, D), jnp.float32)
    total_up = jnp.zeros((F, D), jnp.float32)
    total_down = jnp.zeros((F, D), jnp.float32)
    for set_index in range(set_count):
        lower = set_index * set_rows
        upper = lower + set_rows
        rows_in = picked[lower:upper]
        part_gate = jnp.dot(delta_gate[lower:upper].T, rows_in, preferred_element_type=jnp.float32)
        part_up = jnp.dot(delta_up[lower:upper].T, rows_in, preferred_element_type=jnp.float32)
        part_down = unscale * jnp.dot(hidden[lower:upper].T, cotangent[lower:upper], preferred_element_type=jnp.float32)
        total_gate = total_gate + part_gate.astype(jnp.bfloat16).astype(jnp.float32)
        total_up = total_up + part_up.astype(jnp.bfloat16).astype(jnp.float32)
        total_down = total_down + part_down.astype(jnp.bfloat16).astype(jnp.float32)
    grad_gate_up = jnp.stack([total_gate, total_up]).astype(jnp.bfloat16)
    grad_down = total_down.astype(jnp.bfloat16)
    return grad_gate_up, grad_down
```

```python
import functools

import jax
import jax.numpy as jnp
from jax import lax
from jax.experimental import pallas as pl
from jax.experimental.pallas import tpu as pltpu
from jax.sharding import PartitionSpec as P

MESH = pl.DeviceIdType.MESH
NT = (((1,), (1,)), ((), ()))
NN = (((1,), (0,)), ((), ()))
CHUNKS = 2


def line_of(wide_count):
    bits = wide_count.bit_length() - 1
    near_bits = bits - bits // 2
    return wide_count // 2**near_bits, near_bits


def low_bit(mask, bits):
    return (mask & -mask).bit_length() - 1 if mask else bits


def dot(left_side, right_side, dims):
    return lax.dot_general(left_side, right_side, dims, preferred_element_type=jnp.float32)


def token_plan(near_bits):
    near = 2**near_bits
    sends = [("x", 0, 0)]
    for rel in range(2):
        for mask in range(near):
            sends += [(rel, mask, bit) for bit in range(low_bit(mask, near_bits))]
    masks = [mask for mask in range(2, near, 2)]
    masks.sort(key=lambda mask: (bin(mask).count("1"), -mask))
    keyed = [(0, mask) for mask in masks] + [(1, mask) for mask in [0] + masks]
    keyed.sort(key=lambda item: bin(item[1]).count("1") * 2 + (item[0] * 2 if item[1] else 0))
    relays = [(1 + 2 * CHUNKS * (index // 2), rel, mask) for index, (rel, mask) in enumerate(keyed)]
    return sends, relays


def kernel(
    near_bits,
    rows,
    ids_ref,
    expo_ref,
    pool_ref,
    cot_ref,
    gate_up_ref,
    down_ref,
    out_ref,
    tok_x,
    tok_c,
    far_x,
    pool_buf,
    weights,
    grads,
    from_left,
    from_right,
    own_part,
    sent_part,
    got_part,
    deltas,
    acc,
    out_buf,
    send_w,
    recv_w,
    send_t,
    recv_t,
    send_p,
    recv_p,
    send_g,
    recv_g,
    local_sem,
    pool_sem,
    out_sem,
):
    near = 2**near_bits
    wide_count = rows * near
    grp = lax.axis_index("grp")
    wide = lax.axis_index("wide")
    other = 1 - grp
    row = wide // near
    slot = wide % near
    last = rows - 1
    per_dev, _ = ids_ref.shape
    pool_rows = pool_ref.shape[0]
    half = tok_x.shape[1]
    units = gate_up_ref.shape[1]
    span = rows * units
    group_rows = max(1, min(rows, 128 // units))
    groups = rows // group_rows
    lanes = group_rows * units
    cut = per_dev // CHUNKS
    block = 2 * per_dev
    tile = 512

    bit_of = [(slot // 2**bit) % 2 for bit in range(near_bits)]

    def flipped(mask):
        place = slot
        for bit in range(near_bits):
            if mask >> bit & 1:
                place = place + 2**bit * (1 - 2 * bit_of[bit])
        return place

    across = {"grp": other}
    left = {"wide": jnp.maximum(wide - near, 0)}
    right = {"wide": jnp.minimum(wide + near, wide_count - 1)}
    partner = [{"wide": row * near + flipped(2**bit)} for bit in range(near_bits)]

    barrier = pltpu.get_barrier_semaphore()

    def greet(device):
        pl.semaphore_signal(barrier, inc=1, device_id=device, device_id_type=MESH)

    for device in [across] + partner:
        greet(device)

    @pl.when(row > 0)
    def _():
        greet(left)

    @pl.when(row < last)
    def _():
        greet(right)

    neighbours = (row + last) // rows + (2 * last - row) // rows
    pl.semaphore_wait(barrier, 1 + near_bits + neighbours)

    def remote(source, target, sent, received, device):
        return pltpu.make_async_remote_copy(
            src_ref=source,
            dst_ref=target,
            send_sem=sent,
            recv_sem=received,
            device_id=device,
            device_id_type=MESH,
        )

    def unit_rows(origin):
        return pl.ds(pl.multiple_of(origin * units, units), units)

    def weight_copy(direction, hop, kind, source=None):
        going_right = direction == 0
        origin = row - hop if going_right else row + hop
        origin = jnp.clip(origin, 0, last)
        place = weights.at[kind, unit_rows(origin)]
        return remote(
            place if source is None else source,
            place,
            send_w.at[direction, hop, kind],
            recv_w.at[direction, hop, kind],
            right if going_right else left,
        )

    def weight_sends(direction, hop):
        going_right = direction == 0
        held = row >= hop if going_right else row <= last - hop
        open_end = row < last if going_right else row > 0
        return jnp.logical_and(held, open_end)

    def weight_arrives(direction, hop):
        return row >= hop + 1 if direction == 0 else row <= last - hop - 1

    def weight_arrival(direction, hop, kind):
        origin = row - hop - 1 if direction == 0 else row + hop + 1
        place = weights.at[kind, unit_rows(jnp.clip(origin, 0, last))]
        device = left if direction == 0 else right
        return remote(
            place, place, send_w.at[direction, hop, kind], recv_w.at[direction, hop, kind], device
        )

    def weight_source(kind):
        return gate_up_ref.at[kind] if kind < 2 else down_ref

    for kind in range(3):
        for direction in range(2):

            @pl.when(weight_sends(direction, 0))
            def _(kind=kind, direction=direction):
                weight_copy(direction, 0, kind, weight_source(kind)).start()

    sends, relays = token_plan(near_bits)
    send_index = {key: index for index, key in enumerate(sends)}
    buffers = (tok_c, tok_x)

    def token_rows(rel, mask, chunk):
        base = (grp if rel == 0 else other) * near + flipped(mask)
        return pl.ds(pl.multiple_of(base * per_dev + chunk * cut, cut), cut)

    def token_copy(array, chunk, key, source=None):
        rel, mask, bit = key
        if rel == "x":
            place = buffers[array].at[token_rows(0, 0, chunk)]
            device, arrives = across, near
        else:
            place = buffers[array].at[token_rows(rel, mask, chunk)]
            device, arrives = partner[bit], rel * near + mask + 2**bit
        return remote(
            place if source is None else source,
            place,
            send_t.at[array, chunk, send_index[key]],
            recv_t.at[array, chunk, arrives],
            device,
        )

    def token_arrival(array, chunk, rel, mask):
        place = buffers[array].at[token_rows(rel, mask, chunk)]
        device = across if mask == 0 else partner[low_bit(mask, near_bits)]
        return remote(
            place,
            place,
            send_t.at[array, chunk, 0],
            recv_t.at[array, chunk, rel * near + mask],
            device,
        )

    def half_of(which):
        return pl.ds(pl.multiple_of(which * half, half), half)

    pool_far = pltpu.make_async_copy(pool_ref.at[:, half_of(other)], pool_buf, pool_sem.at[0])
    pool_far.start()
    for chunk in range(CHUNKS):
        piece = pl.ds(chunk * cut, cut)
        token_copy(0, chunk, ("x", 0, 0), cot_ref.at[piece, half_of(other)]).start()
        for bit in reversed(range(near_bits)):
            token_copy(0, chunk, (0, 0, bit), cot_ref.at[piece, half_of(grp)]).start()
    local = [
        pltpu.make_async_copy(
            weight_source(kind), weights.at[kind, unit_rows(row)], local_sem.at[kind]
        )
        for kind in range(3)
    ]
    own_rows = pl.ds(pl.multiple_of((grp * near + slot) * per_dev, per_dev), per_dev)
    local.append(
        pltpu.make_async_copy(cot_ref.at[:, half_of(grp)], tok_c.at[own_rows], local_sem.at[3])
    )
    for copy in local:
        copy.start()

    first_row = (grp * wide_count + wide) * pool_rows
    named = ids_ref[...] - first_row
    pick = (named == lax.broadcasted_iota(jnp.int32, (per_dev, pool_rows), 1)).astype(jnp.bfloat16)

    def pick_into(target, offset):
        @pl.loop(0, half // tile)
        def _(index):
            columns = pl.ds(pl.multiple_of(index * tile, tile), tile)
            target[pl.ds(offset, per_dev), columns] = dot(pick, pool_buf[:, columns], NN).astype(
                jnp.bfloat16
            )

    pool_far.wait()
    pick_into(far_x, 0)
    pool_own = pltpu.make_async_copy(pool_ref.at[:, half_of(grp)], pool_buf, pool_sem.at[1])
    pool_own.start()
    for chunk in range(CHUNKS):
        token_copy(1, chunk, ("x", 0, 0), far_x.at[pl.ds(chunk * cut, cut)]).start()
    pool_own.wait()
    pick_into(tok_x, pl.multiple_of((grp * near + slot) * per_dev, per_dev))
    for chunk in range(CHUNKS):
        for bit in reversed(range(near_bits)):
            token_copy(1, chunk, (0, 0, bit)).start()
    for copy in local:
        copy.wait()

    exponent = expo_ref[0]
    unscale = jnp.float32(1.0)
    for bit in range(4):
        factor = jnp.where((exponent // 2**bit) % 2 == 1, jnp.float32(0.5 ** (2**bit)), jnp.float32(1.0))
        unscale = unscale * factor

    own_group = row // group_rows

    def group_at(order):
        return (own_group + order) % groups

    def group_span(order):
        return pl.ds(pl.multiple_of(group_at(order) * lanes, lanes), lanes)

    blocks = [(rel, mask) for rel in range(2) for mask in range(0, near, 2)]

    def part_copy(order, rel, mask, outgoing=True):
        where = block_rows(rel, mask)
        received = (1 - rel if outgoing else rel, mask)
        return remote(
            sent_part.at[order, where],
            got_part.at[order, where],
            send_p.at[order, blocks.index((rel, mask))],
            recv_p.at[order, blocks.index(received)],
            across,
        )

    def block_rows(rel, mask):
        base = (grp if rel == 0 else other) * near + flipped(mask) - bit_of[0]
        return pl.ds(pl.multiple_of(base * per_dev, block), block)

    def forward(order, rel, mask):
        where = block_rows(rel, mask)
        hidden = group_span(order)
        pair = weights[0:2, hidden, :].reshape(2 * lanes, half)
        acts = dot(tok_x[where, :], pair, NT)
        down = dot(tok_c[where, :], weights[2, hidden, :], NT)
        own_part[order, where, 0 : 2 * lanes] = acts
        own_part[order, where, 2 * lanes : 3 * lanes] = down
        sent_part[order, where, 0 : 2 * lanes] = acts.astype(jnp.bfloat16)
        sent_part[order, where, 2 * lanes : 3 * lanes] = down.astype(jnp.bfloat16)
        part_copy(order, rel, mask).start()

    def backward_deltas(order, rel, mask):
        where = block_rows(rel, mask)
        part_copy(order, rel, mask, False).wait_recv()
        total = own_part[order, where, :] + got_part[order, where, :].astype(jnp.float32)
        gate_act, up_act = total[:, :lanes], total[:, lanes : 2 * lanes]
        delta_hidden = unscale * total[:, 2 * lanes :]
        sig = jax.nn.sigmoid(gate_act)
        made = (
            delta_hidden * up_act * sig * (1.0 + gate_act * (1.0 - sig)),
            delta_hidden * gate_act * sig,
            gate_act * sig * up_act,
        )
        for kind in range(3):
            deltas[kind * lanes : (kind + 1) * lanes, where] = made[kind].T.astype(jnp.bfloat16)

    def weight_grads(order):
        hidden = group_span(order)

        @pl.loop(0, half // tile)
        def _(index):
            columns = pl.ds(pl.multiple_of(index * tile, tile), tile)
            pair = dot(deltas[: 2 * lanes, :], tok_x[:, columns], NN).astype(jnp.bfloat16)
            grads[0, hidden, columns] = pair[:lanes]
            grads[1, hidden, columns] = pair[lanes:]
            down = unscale * dot(deltas[2 * lanes :, :], tok_c[:, columns], NN)
            grads[2, hidden, columns] = down.astype(jnp.bfloat16)

    def await_sibling(rel, mask):
        for array in range(2):
            for chunk in range(CHUNKS):
                token_arrival(array, chunk, rel, mask + 1).wait_recv()

    ready = {(0, 0): 0}
    steps = 3 * last
    for start, rel, mask in relays:
        ready[(rel, mask)] = start + 2 * CHUNKS - 1
        steps = max(steps, ready[(rel, mask)])
    own_ready = 3 * (group_rows - 1)
    done_forward, done_deltas = [], []
    for step in range(1, steps + 1):
        if step <= 3 * last:
            hop, kind = divmod(step - 1, 3)
            for direction in range(2):

                @pl.when(weight_arrives(direction, hop))
                def _(direction=direction, hop=hop, kind=kind):
                    weight_arrival(direction, hop, kind).wait_recv()

                if hop + 1 < last:

                    @pl.when(
                        jnp.logical_and(
                            weight_arrives(direction, hop), weight_sends(direction, hop + 1)
                        )
                    )
                    def _(direction=direction, hop=hop, kind=kind):
                        weight_copy(direction, hop + 1, kind).start()

        for start, rel, mask in relays:
            if start <= step < start + 2 * CHUNKS:
                array, chunk = divmod(step - start, CHUNKS)
                token_arrival(array, chunk, rel, mask).wait_recv()
                for bit in reversed(range(low_bit(mask, near_bits))):
                    token_copy(array, chunk, (rel, mask, bit)).start()
        for key in done_forward:
            if key not in done_deltas and (1 - key[0], key[1]) in done_forward:
                backward_deltas(0, *key)
                done_deltas.append(key)
        if step >= own_ready + 1:
            for key in blocks:
                if key not in done_forward and ready[key] <= step:
                    await_sibling(*key)
                    forward(0, *key)
                    done_forward.append(key)
    for key in blocks:
        if key not in done_forward:
            await_sibling(*key)
            forward(0, *key)
            done_forward.append(key)
    for key in blocks:
        if key not in done_deltas:
            backward_deltas(0, *key)
    weight_grads(0)

    grad_cuts = max(1, units // 32)
    grad_rows = units // grad_cuts

    def grad_place(unit, index):
        kind, part = index // grad_cuts, index % grad_cuts
        start = unit * units + part * grad_rows
        return kind, pl.ds(pl.multiple_of(start, grad_rows), grad_rows)

    def pass_on(going_left, unit, index):
        kind, where = grad_place(unit, index)
        landing = from_right if going_left else from_left
        direction = 0 if going_left else 1
        copy = remote(
            grads.at[kind, where],
            landing.at[kind, where],
            send_g.at[direction, unit, index],
            recv_g.at[direction, unit, index],
            left if going_left else right,
        )

        @pl.when(row < last if going_left else row > 0)
        def _():
            copy.wait_recv()
            summed = grads[kind, where, :].astype(jnp.float32) + landing[kind, where, :].astype(
                jnp.float32
            )
            grads[kind, where, :] = summed.astype(jnp.bfloat16)

        copy.start()

    def pass_units(unit):
        mirror = last - unit

        @pl.loop(0, 3 * grad_cuts)
        def _(index):
            @pl.when(jnp.logical_and(row > unit, row >= rows // 2))
            def _():
                pass_on(True, unit, index)

            @pl.when(row < mirror)
            def _():
                pass_on(False, mirror, index)

            @pl.when(jnp.logical_and(row > unit, row < rows // 2))
            def _():
                pass_on(True, unit, index)

    order_left = [last - 1] + list(range(last - 1))
    if group_rows > 1:
        pass_units(order_left[0])
    for order in range(1, groups):
        for key in blocks:
            forward(order, *key)
        for key in blocks:
            backward_deltas(order, *key)
        weight_grads(order)
    if group_rows == 1:
        pass_units(order_left[0])
    for unit in order_left[1:]:
        pass_units(unit)

    def out_copy(index):
        kind, part = index // grad_cuts, index % grad_cuts
        where = pl.ds(pl.multiple_of(part * grad_rows, grad_rows), grad_rows)
        return pltpu.make_async_copy(
            out_buf.at[kind, where], out_ref.at[kind, where], out_sem.at[index]
        )

    @pl.loop(0, 3 * grad_cuts)
    def _(index):
        kind, where = grad_place(row, index)
        acc[...] = grads[kind, where, :].astype(jnp.float32)
        for direction, landing, present in ((1, from_left, row > 0), (0, from_right, row < last)):

            @pl.when(present)
            def _(direction=direction, landing=landing):
                place = landing.at[kind, where]
                remote(
                    place,
                    place,
                    send_g.at[direction, row, index],
                    recv_g.at[direction, row, index],
                    across,
                ).wait_recv()
                acc[...] += landing[kind, where, :].astype(jnp.float32)

        part = index % grad_cuts
        to = pl.ds(pl.multiple_of(part * grad_rows, grad_rows), grad_rows)
        out_buf[kind, to, :] = acc[...].astype(jnp.bfloat16)
        out_copy(index).start()

    for kind in range(3):
        for direction in range(2):
            for hop in range(last):

                @pl.when(weight_sends(direction, hop))
                def _(kind=kind, direction=direction, hop=hop):
                    weight_copy(direction, hop, kind).wait_send()

    for array in range(2):
        for chunk in range(CHUNKS):
            for key in sends:
                token_copy(array, chunk, key).wait_send()
    for order in range(groups):
        for key in blocks:
            part_copy(order, *key).wait_send()

    @pl.loop(0, 3 * grad_cuts)
    def _(index):
        for unit in range(rows):
            kind, where = grad_place(unit, index)
            place = grads.at[kind, where]
            for direction, goes in ((0, row > unit), (1, row < unit)):

                @pl.when(goes)
                def _(direction=direction, unit=unit, place=place):
                    remote(
                        place,
                        place,
                        send_g.at[direction, unit, index],
                        recv_g.at[direction, unit, index],
                        across,
                    ).wait_send()

        out_copy(index).wait()


def per_device(rows, near_bits, x_pool, token_ids, cotangent, gate_up, down_weight, loss_exponent):
    near = 2**near_bits
    _, units, half = gate_up.shape
    per_dev = token_ids.shape[0]
    span = rows * units
    group_rows = max(1, min(rows, 128 // units))
    groups, lanes = rows // group_rows, group_rows * units
    token_count = 2 * near * per_dev
    grad_cuts = max(1, units // 32)
    sends, _ = token_plan(near_bits)
    bf16, f32 = jnp.bfloat16, jnp.float32
    anywhere = pl.BlockSpec(memory_space=pl.ANY)
    dma = pltpu.SemaphoreType.DMA
    blocks = near
    out = pl.pallas_call(
        functools.partial(kernel, near_bits, rows),
        out_shape=jax.ShapeDtypeStruct((3, units, half), bf16),
        in_specs=[
            pl.BlockSpec(memory_space=pltpu.VMEM),
            pl.BlockSpec(memory_space=pltpu.SMEM),
            anywhere,
            anywhere,
            anywhere,
            anywhere,
        ],
        out_specs=anywhere,
        scratch_shapes=[
            pltpu.VMEM((token_count, half), bf16),
            pltpu.VMEM((token_count, half), bf16),
            pltpu.VMEM((per_dev, half), bf16),
            pltpu.VMEM((x_pool.shape[0], half), bf16),
            pltpu.VMEM((3, span, half), bf16),
            pltpu.VMEM((3, span, half), bf16),
            pltpu.VMEM((3, span, half), bf16),
            pltpu.VMEM((3, span, half), bf16),
            pltpu.VMEM((groups, token_count, 3 * lanes), f32),
            pltpu.VMEM((groups, token_count, 3 * lanes), bf16),
            pltpu.VMEM((groups, token_count, 3 * lanes), bf16),
            pltpu.VMEM((3 * lanes, token_count), bf16),
            pltpu.VMEM((units // grad_cuts, half), f32),
            pltpu.VMEM((3, units, half), bf16),
            dma((2, rows - 1, 3)),
            dma((2, rows - 1, 3)),
            dma((2, CHUNKS, len(sends))),
            dma((2, CHUNKS, 2 * near)),
            dma((groups, blocks)),
            dma((groups, blocks)),
            dma((2, rows, 3 * grad_cuts)),
            dma((2, rows, 3 * grad_cuts)),
            dma((4,)),
            dma((2,)),
            dma((3 * grad_cuts,)),
        ],
        compiler_params=pltpu.CompilerParams(
            collective_id=0, has_side_effects=True, vmem_limit_bytes=67_000_000
        ),
    )(token_ids.reshape(per_dev, 1), loss_exponent, x_pool, cotangent, gate_up, down_weight)
    return out[:2], out[2]


def solution(mesh):
    rows, near_bits = line_of(mesh.shape["wide"])
    return jax.shard_map(
        functools.partial(per_device, rows, near_bits),
        mesh=mesh,
        in_specs=(
            P(("grp", "wide"), None),
            P(("grp", "wide")),
            P(("grp", "wide"), None),
            P(None, "wide", "grp"),
            P("wide", "grp"),
            P(),
        ),
        out_specs=(P(None, "wide", "grp"), P("wide", "grp")),
        check_vma=False,
    )
```

```python
import functools

import jax
import jax.numpy as jnp
from jax import lax
from jax.experimental import pallas as pl
from jax.experimental.pallas import tpu as pltpu
from jax.sharding import PartitionSpec as P

MESH = pl.DeviceIdType.MESH
NT = (((1,), (1,)), ((), ()))
NN = (((1,), (0,)), ((), ()))
CHUNKS = 2


def line_of(wide_count):
    bits = wide_count.bit_length() - 1
    near_bits = bits - bits // 2
    return wide_count // 2**near_bits, near_bits


def low_bit(mask, bits):
    return (mask & -mask).bit_length() - 1 if mask else bits


def dot(left_side, right_side, dims):
    return lax.dot_general(left_side, right_side, dims, preferred_element_type=jnp.float32)


def token_plan(near_bits):
    near = 2**near_bits
    sends = [("x", 0, 0)]
    for rel in range(2):
        for mask in range(near):
            sends += [(rel, mask, bit) for bit in range(low_bit(mask, near_bits))]
    masks = [mask for mask in range(2, near, 2)]
    masks.sort(key=lambda mask: (bin(mask).count("1"), -mask))
    keyed = [(0, mask) for mask in masks] + [(1, mask) for mask in [0] + masks]
    keyed.sort(key=lambda item: bin(item[1]).count("1") * 2 + (item[0] * 2 if item[1] else 0))
    relays = [(1 + 2 * CHUNKS * (index // 2), rel, mask) for index, (rel, mask) in enumerate(keyed)]
    return sends, relays


def kernel(
    near_bits,
    rows,
    ids_ref,
    expo_ref,
    pool_ref,
    cot_ref,
    gate_up_ref,
    down_ref,
    pair_out,
    down_out,
    tok_x,
    tok_c,
    far_x,
    pool_buf,
    weights,
    grads,
    from_left,
    from_right,
    own_part,
    sent_part,
    got_part,
    deltas,
    acc,
    out_buf,
    send_w,
    recv_w,
    send_t,
    recv_t,
    send_p,
    recv_p,
    send_g,
    recv_g,
    local_sem,
    pool_sem,
    out_sem,
):
    near = 2**near_bits
    wide_count = rows * near
    grp = lax.axis_index("grp")
    wide = lax.axis_index("wide")
    other = 1 - grp
    row = wide // near
    slot = wide % near
    last = rows - 1
    per_dev = ids_ref.shape[1]
    pool_rows = pool_ref.shape[0]
    half = tok_x.shape[1]
    units = gate_up_ref.shape[1]
    span = rows * units
    group_rows = max(1, min(rows, 128 // units))
    groups = rows // group_rows
    lanes = group_rows * units
    cut = per_dev // CHUNKS
    block = 2 * per_dev
    tile = 512

    bit_of = [(slot // 2**bit) % 2 for bit in range(near_bits)]

    def flipped(mask):
        place = slot
        for bit in range(near_bits):
            if mask >> bit & 1:
                place = place + 2**bit * (1 - 2 * bit_of[bit])
        return place

    across = {"grp": other}
    left = {"wide": jnp.maximum(wide - near, 0)}
    right = {"wide": jnp.minimum(wide + near, wide_count - 1)}
    partner = [{"wide": row * near + flipped(2**bit)} for bit in range(near_bits)]

    barrier = pltpu.get_barrier_semaphore()

    def greet(device):
        pl.semaphore_signal(barrier, inc=1, device_id=device, device_id_type=MESH)

    for device in [across] + partner:
        greet(device)

    @pl.when(row > 0)
    def _():
        greet(left)

    @pl.when(row < last)
    def _():
        greet(right)

    neighbours = (row + last) // rows + (2 * last - row) // rows
    pl.semaphore_wait(barrier, 1 + near_bits + neighbours)

    def remote(source, target, sent, received, device):
        return pltpu.make_async_remote_copy(
            src_ref=source,
            dst_ref=target,
            send_sem=sent,
            recv_sem=received,
            device_id=device,
            device_id_type=MESH,
        )

    def unit_rows(origin):
        return pl.ds(pl.multiple_of(origin * units, units), units)

    def weight_copy(direction, hop, kind, source=None):
        going_right = direction == 0
        origin = row - hop if going_right else row + hop
        origin = jnp.clip(origin, 0, last)
        place = weights.at[kind, unit_rows(origin)]
        return remote(
            place if source is None else source,
            place,
            send_w.at[direction, hop, kind],
            recv_w.at[direction, hop, kind],
            right if going_right else left,
        )

    def weight_sends(direction, hop):
        going_right = direction == 0
        held = row >= hop if going_right else row <= last - hop
        open_end = row < last if going_right else row > 0
        return jnp.logical_and(held, open_end)

    def weight_arrives(direction, hop):
        return row >= hop + 1 if direction == 0 else row <= last - hop - 1

    def weight_arrival(direction, hop, kind):
        origin = row - hop - 1 if direction == 0 else row + hop + 1
        place = weights.at[kind, unit_rows(jnp.clip(origin, 0, last))]
        device = left if direction == 0 else right
        return remote(
            place, place, send_w.at[direction, hop, kind], recv_w.at[direction, hop, kind], device
        )

    def weight_source(kind):
        return gate_up_ref.at[kind] if kind < 2 else down_ref

    for kind in range(3):
        for direction in range(2):

            @pl.when(weight_sends(direction, 0))
            def _(kind=kind, direction=direction):
                weight_copy(direction, 0, kind, weight_source(kind)).start()

    sends, relays = token_plan(near_bits)
    send_index = {key: index for index, key in enumerate(sends)}
    buffers = (tok_c, tok_x)

    def token_rows(rel, mask, chunk):
        base = (grp if rel == 0 else other) * near + flipped(mask)
        return pl.ds(pl.multiple_of(base * per_dev + chunk * cut, cut), cut)

    def token_copy(array, chunk, key, source=None):
        rel, mask, bit = key
        if rel == "x":
            place = buffers[array].at[token_rows(0, 0, chunk)]
            device, arrives = across, near
        else:
            place = buffers[array].at[token_rows(rel, mask, chunk)]
            device, arrives = partner[bit], rel * near + mask + 2**bit
        return remote(
            place if source is None else source,
            place,
            send_t.at[array, chunk, send_index[key]],
            recv_t.at[array, chunk, arrives],
            device,
        )

    def token_arrival(array, chunk, rel, mask):
        place = buffers[array].at[token_rows(rel, mask, chunk)]
        device = across if mask == 0 else partner[low_bit(mask, near_bits)]
        return remote(
            place,
            place,
            send_t.at[array, chunk, 0],
            recv_t.at[array, chunk, rel * near + mask],
            device,
        )

    def half_of(which):
        return pl.ds(pl.multiple_of(which * half, half), half)

    pool_far = pltpu.make_async_copy(pool_ref.at[:, half_of(other)], pool_buf, pool_sem.at[0])
    pool_far.start()
    for chunk in range(CHUNKS):
        piece = pl.ds(chunk * cut, cut)
        token_copy(0, chunk, ("x", 0, 0), cot_ref.at[piece, half_of(other)]).start()
        for bit in reversed(range(near_bits)):
            token_copy(0, chunk, (0, 0, bit), cot_ref.at[piece, half_of(grp)]).start()
    local = [
        pltpu.make_async_copy(
            weight_source(kind), weights.at[kind, unit_rows(row)], local_sem.at[kind]
        )
        for kind in range(3)
    ]
    own_rows = pl.ds(pl.multiple_of((grp * near + slot) * per_dev, per_dev), per_dev)
    local.append(
        pltpu.make_async_copy(cot_ref.at[:, half_of(grp)], tok_c.at[own_rows], local_sem.at[3])
    )
    for copy in local:
        copy.start()

    first_row = (grp * wide_count + wide) * pool_rows
    named = (ids_ref[...] - first_row).astype(jnp.float32)
    named = jnp.broadcast_to(named, (per_dev, per_dev)).T.astype(jnp.int32)[:, :1]
    pick = (named == lax.broadcasted_iota(jnp.int32, (per_dev, pool_rows), 1)).astype(jnp.bfloat16)

    def pick_into(target, offset):
        @pl.loop(0, half // tile)
        def _(index):
            columns = pl.ds(pl.multiple_of(index * tile, tile), tile)
            target[pl.ds(offset, per_dev), columns] = dot(pick, pool_buf[:, columns], NN).astype(
                jnp.bfloat16
            )

    pool_far.wait()
    pick_into(far_x, 0)
    pool_own = pltpu.make_async_copy(pool_ref.at[:, half_of(grp)], pool_buf, pool_sem.at[1])
    pool_own.start()
    for chunk in range(CHUNKS):
        token_copy(1, chunk, ("x", 0, 0), far_x.at[pl.ds(chunk * cut, cut)]).start()
    pool_own.wait()
    pick_into(tok_x, pl.multiple_of((grp * near + slot) * per_dev, per_dev))
    for chunk in range(CHUNKS):
        for bit in reversed(range(near_bits)):
            token_copy(1, chunk, (0, 0, bit)).start()
    for copy in local:
        copy.wait()

    exponent = expo_ref[0]
    unscale = jnp.float32(1.0)
    for bit in range(4):
        factor = jnp.where((exponent // 2**bit) % 2 == 1, jnp.float32(0.5 ** (2**bit)), jnp.float32(1.0))
        unscale = unscale * factor

    own_group = row // group_rows

    def group_at(order):
        return (own_group + order) % groups

    def group_span(order):
        return pl.ds(pl.multiple_of(group_at(order) * lanes, lanes), lanes)

    blocks = [(rel, mask) for rel in range(2) for mask in range(0, near, 2)]

    def part_copy(order, rel, mask, outgoing=True):
        where = block_rows(rel, mask)
        received = (1 - rel if outgoing else rel, mask)
        return remote(
            sent_part.at[order, where],
            got_part.at[order, where],
            send_p.at[order, blocks.index((rel, mask))],
            recv_p.at[order, blocks.index(received)],
            across,
        )

    def block_rows(rel, mask):
        base = (grp if rel == 0 else other) * near + flipped(mask) - bit_of[0]
        return pl.ds(pl.multiple_of(base * per_dev, block), block)

    def forward(order, rel, mask):
        where = block_rows(rel, mask)
        hidden = group_span(order)
        pair = weights[0:2, hidden, :].reshape(2 * lanes, half)
        acts = dot(tok_x[where, :], pair, NT)
        down = dot(tok_c[where, :], weights[2, hidden, :], NT)
        own_part[order, where, 0 : 2 * lanes] = acts
        own_part[order, where, 2 * lanes : 3 * lanes] = down
        sent_part[order, where, 0 : 2 * lanes] = acts.astype(jnp.bfloat16)
        sent_part[order, where, 2 * lanes : 3 * lanes] = down.astype(jnp.bfloat16)
        part_copy(order, rel, mask).start()

    def backward_deltas(order, rel, mask):
        where = block_rows(rel, mask)
        part_copy(order, rel, mask, False).wait_recv()
        total = own_part[order, where, :] + got_part[order, where, :].astype(jnp.float32)
        gate_act, up_act = total[:, :lanes], total[:, lanes : 2 * lanes]
        delta_hidden = unscale * total[:, 2 * lanes :]
        sig = jax.nn.sigmoid(gate_act)
        made = (
            delta_hidden * up_act * sig * (1.0 + gate_act * (1.0 - sig)),
            delta_hidden * gate_act * sig,
            gate_act * sig * up_act,
        )
        for kind in range(3):
            deltas[kind * lanes : (kind + 1) * lanes, where] = made[kind].T.astype(jnp.bfloat16)

    def pair_grads(order):
        hidden = group_span(order)

        @pl.loop(0, half // tile)
        def _(index):
            columns = pl.ds(pl.multiple_of(index * tile, tile), tile)
            pair = dot(deltas[: 2 * lanes, :], tok_x[:, columns], NN).astype(jnp.bfloat16)
            grads[0, hidden, columns] = pair[:lanes]
            grads[1, hidden, columns] = pair[lanes:]

    def down_grads(order):
        hidden = group_span(order)

        @pl.loop(0, half // tile)
        def _(index):
            columns = pl.ds(pl.multiple_of(index * tile, tile), tile)
            down = unscale * dot(deltas[2 * lanes :, :], tok_c[:, columns], NN)
            grads[2, hidden, columns] = down.astype(jnp.bfloat16)

    def await_sibling(rel, mask):
        for array in range(2):
            for chunk in range(CHUNKS):
                token_arrival(array, chunk, rel, mask + 1).wait_recv()

    ready = {(0, 0): 0}
    deferred = groups > 1
    weight_steps = 3 * (last - 1) if deferred else 3 * last
    steps = weight_steps
    for start, rel, mask in relays:
        ready[(rel, mask)] = start + 2 * CHUNKS - 1
        steps = max(steps, ready[(rel, mask)])
    own_ready = 3 * (group_rows - 1)
    done_forward, done_deltas = [], []
    for step in range(1, steps + 1):
        if step <= weight_steps:
            hop, kind = divmod(step - 1, 3)
            for direction in range(2):

                @pl.when(weight_arrives(direction, hop))
                def _(direction=direction, hop=hop, kind=kind):
                    weight_arrival(direction, hop, kind).wait_recv()

                if hop + 1 < last:

                    @pl.when(
                        jnp.logical_and(
                            weight_arrives(direction, hop), weight_sends(direction, hop + 1)
                        )
                    )
                    def _(direction=direction, hop=hop, kind=kind):
                        weight_copy(direction, hop + 1, kind).start()

        for start, rel, mask in relays:
            if start <= step < start + 2 * CHUNKS:
                array, chunk = divmod(step - start, CHUNKS)
                token_arrival(array, chunk, rel, mask).wait_recv()
                for bit in reversed(range(low_bit(mask, near_bits))):
                    token_copy(array, chunk, (rel, mask, bit)).start()
        for key in done_forward:
            if key not in done_deltas and (1 - key[0], key[1]) in done_forward:
                backward_deltas(0, *key)
                done_deltas.append(key)
        if step >= own_ready + 1:
            for key in blocks:
                if key not in done_forward and ready[key] <= step:
                    await_sibling(*key)
                    forward(0, *key)
                    done_forward.append(key)
    for key in blocks:
        if key not in done_forward:
            await_sibling(*key)
            forward(0, *key)
            done_forward.append(key)
    for key in blocks:
        if key not in done_deltas:
            backward_deltas(0, *key)
    down_grads(0)

    grad_cuts = max(1, units // 32)
    grad_rows = units // grad_cuts

    def grad_place(unit, index):
        kind, part = (index // grad_cuts + 2) % 3, index % grad_cuts
        start = unit * units + part * grad_rows
        return kind, pl.ds(pl.multiple_of(start, grad_rows), grad_rows)

    def pass_on(going_left, unit, index):
        kind, where = grad_place(unit, index)
        landing = from_right if going_left else from_left
        direction = 0 if going_left else 1
        copy = remote(
            grads.at[kind, where],
            landing.at[kind, where],
            send_g.at[direction, unit, index],
            recv_g.at[direction, unit, index],
            left if going_left else right,
        )

        @pl.when(row < last if going_left else row > 0)
        def _():
            copy.wait_recv()
            summed = grads[kind, where, :].astype(jnp.float32) + landing[kind, where, :].astype(
                jnp.float32
            )
            grads[kind, where, :] = summed.astype(jnp.bfloat16)

        copy.start()

    def out_copy(index):
        kind, part = (index // grad_cuts + 2) % 3, index % grad_cuts
        to = pl.ds(pl.multiple_of(part * grad_rows, grad_rows), grad_rows)
        pair = pltpu.make_async_copy(
            out_buf.at[kind, to], pair_out.at[kind % 2, to], out_sem.at[index]
        )
        down = pltpu.make_async_copy(out_buf.at[kind, to], down_out.at[to], out_sem.at[index])
        return kind, to, pair, down

    def finish(index):
        kind, where = grad_place(row, index)
        acc[...] = grads[kind, where, :].astype(jnp.float32)
        for direction, landing, present in ((1, from_left, row > 0), (0, from_right, row < last)):

            @pl.when(present)
            def _(direction=direction, landing=landing):
                place = landing.at[kind, where]
                remote(
                    place,
                    place,
                    send_g.at[direction, row, index],
                    recv_g.at[direction, row, index],
                    across,
                ).wait_recv()
                acc[...] += landing[kind, where, :].astype(jnp.float32)

        _, to, pair, down = out_copy(index)
        out_buf[kind, to, :] = acc[...].astype(jnp.bfloat16)

        @pl.when(kind < 2)
        def _():
            pair.start()

        @pl.when(kind == 2)
        def _():
            down.start()

    upper = row >= rows // 2
    lower = row < rows // 2

    def pass_units(unit, first=0, end=3, finishing=False):
        mirror = last - unit
        first, end = first * grad_cuts, end * grad_cuts

        @pl.loop(first, end + 1)
        def _(index):
            now, later = index < end, index > first

            @pl.when(jnp.logical_and(jnp.logical_and(upper, row > unit), now))
            def _():
                pass_on(True, unit, index)

            @pl.when(jnp.logical_and(jnp.logical_and(lower, row < mirror), now))
            def _():
                pass_on(False, mirror, index)

            @pl.when(jnp.logical_and(jnp.logical_and(upper, row < mirror), later))
            def _():
                pass_on(False, mirror, index - 1)

            @pl.when(jnp.logical_and(jnp.logical_and(lower, row > unit), later))
            def _():
                pass_on(True, unit, index - 1)

            if finishing:

                @pl.when(later)
                def _():
                    finish(index - 1)

    order_left = [last - 1] + list(range(last - 1))
    if group_rows > 1:
        pass_units(order_left[0], 0, 1, last == 1)
    pair_grads(0)
    if group_rows > 1:
        pass_units(order_left[0], 1, 3, last == 1)
    if deferred:
        for kind in range(3):
            for direction in range(2):

                @pl.when(weight_arrives(direction, last - 1))
                def _(direction=direction, kind=kind):
                    weight_arrival(direction, last - 1, kind).wait_recv()

    for order in range(1, groups):
        for key in blocks:
            forward(order, *key)
        for key in blocks:
            backward_deltas(order, *key)
        down_grads(order)
        pair_grads(order)
    if group_rows == 1:
        pass_units(order_left[0])
    for unit in order_left[1:]:
        pass_units(unit, finishing=unit == order_left[-1])

    for kind in range(3):
        for direction in range(2):
            for hop in range(last):

                @pl.when(weight_sends(direction, hop))
                def _(kind=kind, direction=direction, hop=hop):
                    weight_copy(direction, hop, kind).wait_send()

    for array in range(2):
        for chunk in range(CHUNKS):
            for key in sends:
                token_copy(array, chunk, key).wait_send()
    for order in range(groups):
        for key in blocks:
            part_copy(order, *key).wait_send()

    @pl.loop(0, 3 * grad_cuts)
    def _(index):
        for unit in range(rows):
            kind, where = grad_place(unit, index)
            place = grads.at[kind, where]
            for direction, goes in ((0, row > unit), (1, row < unit)):

                @pl.when(goes)
                def _(direction=direction, unit=unit, place=place):
                    remote(
                        place,
                        place,
                        send_g.at[direction, unit, index],
                        recv_g.at[direction, unit, index],
                        across,
                    ).wait_send()

        kind, _, pair, down = out_copy(index)

        @pl.when(kind < 2)
        def _():
            pair.wait()

        @pl.when(kind == 2)
        def _():
            down.wait()


def per_device(rows, near_bits, x_pool, token_ids, cotangent, gate_up, down_weight, loss_exponent):
    near = 2**near_bits
    _, units, half = gate_up.shape
    per_dev = token_ids.shape[0]
    span = rows * units
    group_rows = max(1, min(rows, 128 // units))
    groups, lanes = rows // group_rows, group_rows * units
    token_count = 2 * near * per_dev
    grad_cuts = max(1, units // 32)
    sends, _ = token_plan(near_bits)
    bf16, f32 = jnp.bfloat16, jnp.float32
    anywhere = pl.BlockSpec(memory_space=pl.ANY)
    dma = pltpu.SemaphoreType.DMA
    blocks = near
    out = pl.pallas_call(
        functools.partial(kernel, near_bits, rows),
        out_shape=(
            jax.ShapeDtypeStruct((2, units, half), bf16),
            jax.ShapeDtypeStruct((units, half), bf16),
        ),
        in_specs=[
            pl.BlockSpec(memory_space=pltpu.VMEM),
            pl.BlockSpec(memory_space=pltpu.SMEM),
            anywhere,
            anywhere,
            anywhere,
            anywhere,
        ],
        out_specs=(anywhere, anywhere),
        scratch_shapes=[
            pltpu.VMEM((token_count, half), bf16),
            pltpu.VMEM((token_count, half), bf16),
            pltpu.VMEM((per_dev, half), bf16),
            pltpu.VMEM((x_pool.shape[0], half), bf16),
            pltpu.VMEM((3, span, half), bf16),
            pltpu.VMEM((3, span, half), bf16),
            pltpu.VMEM((3, span, half), bf16),
            pltpu.VMEM((3, span, half), bf16),
            pltpu.VMEM((groups, token_count, 3 * lanes), f32),
            pltpu.VMEM((groups, token_count, 3 * lanes), bf16),
            pltpu.VMEM((groups, token_count, 3 * lanes), bf16),
            pltpu.VMEM((3 * lanes, token_count), bf16),
            pltpu.VMEM((units // grad_cuts, half), f32),
            pltpu.VMEM((3, units, half), bf16),
            dma((2, rows - 1, 3)),
            dma((2, rows - 1, 3)),
            dma((2, CHUNKS, len(sends))),
            dma((2, CHUNKS, 2 * near)),
            dma((groups, blocks)),
            dma((groups, blocks)),
            dma((2, rows, 3 * grad_cuts)),
            dma((2, rows, 3 * grad_cuts)),
            dma((4,)),
            dma((2,)),
            dma((3 * grad_cuts,)),
        ],
        compiler_params=pltpu.CompilerParams(
            collective_id=0, has_side_effects=True, vmem_limit_bytes=67_000_000
        ),
    )(token_ids.reshape(1, per_dev), loss_exponent, x_pool, cotangent, gate_up, down_weight)
    return out


def solution(mesh):
    rows, near_bits = line_of(mesh.shape["wide"])
    return jax.shard_map(
        functools.partial(per_device, rows, near_bits),
        mesh=mesh,
        in_specs=(
            P(("grp", "wide"), None),
            P(("grp", "wide")),
            P(("grp", "wide"), None),
            P(None, "wide", "grp"),
            P("wide", "grp"),
            P(),
        ),
        out_specs=(P(None, "wide", "grp"), P("wide", "grp")),
        check_vma=False,
    )
```

```python
import functools

import jax
import jax.numpy as jnp
from jax import lax
from jax.experimental import pallas as pl
from jax.experimental.pallas import tpu as pltpu
from jax.sharding import PartitionSpec as P

MESH = pl.DeviceIdType.MESH
NT = (((1,), (1,)), ((), ()))
NN = (((1,), (0,)), ((), ()))
CHUNKS = 2


def line_of(wide_count):
    bits = wide_count.bit_length() - 1
    near_bits = bits - bits // 2
    return wide_count // 2**near_bits, near_bits


def low_bit(mask, bits):
    return (mask & -mask).bit_length() - 1 if mask else bits


def dot(left_side, right_side, dims):
    return lax.dot_general(left_side, right_side, dims, preferred_element_type=jnp.float32)


def token_plan(near_bits):
    near = 2**near_bits
    sends = [("x", 0, 0)]
    for rel in range(2):
        for mask in range(near):
            sends += [(rel, mask, bit) for bit in range(low_bit(mask, near_bits))]
    masks = [mask for mask in range(2, near, 2)]
    masks.sort(key=lambda mask: (bin(mask).count("1"), -mask))
    keyed = [(0, mask) for mask in masks] + [(1, mask) for mask in [0] + masks]
    keyed.sort(key=lambda item: bin(item[1]).count("1") * 2 + (item[0] * 2 if item[1] else 0))
    relays = [(1 + 2 * CHUNKS * (index // 2), rel, mask) for index, (rel, mask) in enumerate(keyed)]
    return sends, relays


def kernel(
    near_bits,
    rows,
    ids_ref,
    expo_ref,
    pool_ref,
    cot_ref,
    gate_up_ref,
    down_ref,
    pair_out,
    down_out,
    tok_x,
    tok_c,
    far_x,
    pool_buf,
    weights,
    grads,
    from_left,
    from_right,
    own_part,
    sent_part,
    got_part,
    deltas,
    acc,
    out_buf,
    send_w,
    recv_w,
    send_t,
    recv_t,
    send_p,
    recv_p,
    send_g,
    recv_g,
    local_sem,
    pool_sem,
    out_sem,
):
    near = 2**near_bits
    wide_count = rows * near
    grp = lax.axis_index("grp")
    wide = lax.axis_index("wide")
    other = 1 - grp
    row = wide // near
    slot = wide % near
    last = rows - 1
    per_dev = ids_ref.shape[1]
    pool_rows = pool_ref.shape[0]
    half = tok_x.shape[1]
    units = gate_up_ref.shape[1]
    span = rows * units
    group_rows = max(1, min(rows, 128 // units))
    groups = rows // group_rows
    lanes = group_rows * units
    cut = per_dev // CHUNKS
    block = 2 * per_dev
    tile = 512

    bit_of = [(slot // 2**bit) % 2 for bit in range(near_bits)]

    def flipped(mask):
        place = slot
        for bit in range(near_bits):
            if mask >> bit & 1:
                place = place + 2**bit * (1 - 2 * bit_of[bit])
        return place

    across = {"grp": other}
    left = {"wide": jnp.maximum(wide - near, 0)}
    right = {"wide": jnp.minimum(wide + near, wide_count - 1)}
    partner = [{"wide": row * near + flipped(2**bit)} for bit in range(near_bits)]

    barrier = pltpu.get_barrier_semaphore()

    def greet(device):
        pl.semaphore_signal(barrier, inc=1, device_id=device, device_id_type=MESH)

    for device in [across] + partner:
        greet(device)

    @pl.when(row > 0)
    def _():
        greet(left)

    @pl.when(row < last)
    def _():
        greet(right)

    neighbours = (row + last) // rows + (2 * last - row) // rows
    pl.semaphore_wait(barrier, 1 + near_bits + neighbours)

    def remote(source, target, sent, received, device):
        return pltpu.make_async_remote_copy(
            src_ref=source,
            dst_ref=target,
            send_sem=sent,
            recv_sem=received,
            device_id=device,
            device_id_type=MESH,
        )

    def unit_rows(origin):
        return pl.ds(pl.multiple_of(origin * units, units), units)

    def weight_copy(direction, hop, kind, source=None):
        going_right = direction == 0
        origin = row - hop if going_right else row + hop
        origin = jnp.clip(origin, 0, last)
        place = weights.at[kind, unit_rows(origin)]
        return remote(
            place if source is None else source,
            place,
            send_w.at[direction, hop, kind],
            recv_w.at[direction, hop, kind],
            right if going_right else left,
        )

    def weight_sends(direction, hop):
        going_right = direction == 0
        held = row >= hop if going_right else row <= last - hop
        open_end = row < last if going_right else row > 0
        return jnp.logical_and(held, open_end)

    def weight_arrives(direction, hop):
        return row >= hop + 1 if direction == 0 else row <= last - hop - 1

    def weight_arrival(direction, hop, kind):
        origin = row - hop - 1 if direction == 0 else row + hop + 1
        place = weights.at[kind, unit_rows(jnp.clip(origin, 0, last))]
        device = left if direction == 0 else right
        return remote(
            place, place, send_w.at[direction, hop, kind], recv_w.at[direction, hop, kind], device
        )

    def weight_source(kind):
        return gate_up_ref.at[kind] if kind < 2 else down_ref

    for kind in range(3):
        for direction in range(2):

            @pl.when(weight_sends(direction, 0))
            def _(kind=kind, direction=direction):
                weight_copy(direction, 0, kind, weight_source(kind)).start()

    sends, relays = token_plan(near_bits)
    send_index = {key: index for index, key in enumerate(sends)}
    buffers = (tok_c, tok_x)

    def token_rows(rel, mask, chunk):
        core = bit_of[0] if mask % 2 == 0 else 1 - bit_of[0]
        base = (grp if rel == 0 else other) * near + flipped(mask) - core
        start = base * per_dev + (2 * chunk + core) * cut
        return pl.ds(pl.multiple_of(start, cut), cut)

    def token_copy(array, chunk, key, source=None):
        rel, mask, bit = key
        if rel == "x":
            place = buffers[array].at[token_rows(0, 0, chunk)]
            device, arrives = across, near
        else:
            place = buffers[array].at[token_rows(rel, mask, chunk)]
            device, arrives = partner[bit], rel * near + mask + 2**bit
        return remote(
            place if source is None else source,
            place,
            send_t.at[array, chunk, send_index[key]],
            recv_t.at[array, chunk, arrives],
            device,
        )

    def token_arrival(array, chunk, rel, mask):
        place = buffers[array].at[token_rows(rel, mask, chunk)]
        device = across if mask == 0 else partner[low_bit(mask, near_bits)]
        return remote(
            place,
            place,
            send_t.at[array, chunk, 0],
            recv_t.at[array, chunk, rel * near + mask],
            device,
        )

    def half_of(which):
        return pl.ds(pl.multiple_of(which * half, half), half)

    pool_far = pltpu.make_async_copy(pool_ref.at[:, half_of(other)], pool_buf, pool_sem.at[0])
    pool_far.start()
    for chunk in range(CHUNKS):
        piece = pl.ds(chunk * cut, cut)
        if chunk == 0:
            token_copy(0, chunk, ("x", 0, 0), cot_ref.at[piece, half_of(other)]).start()
        for bit in reversed(range(near_bits)):
            token_copy(0, chunk, (0, 0, bit), cot_ref.at[piece, half_of(grp)]).start()
    local = [
        pltpu.make_async_copy(
            weight_source(kind), weights.at[kind, unit_rows(row)], local_sem.at[kind]
        )
        for kind in range(3)
    ]
    for chunk in range(CHUNKS):
        piece = pl.ds(chunk * cut, cut)
        local.append(
            pltpu.make_async_copy(
                cot_ref.at[piece, half_of(grp)],
                tok_c.at[token_rows(0, 0, chunk)],
                local_sem.at[3 + chunk],
            )
        )
    for copy in local:
        copy.start()

    first_row = (grp * wide_count + wide) * pool_rows
    named = (ids_ref[...] - first_row).astype(jnp.float32)
    named = jnp.broadcast_to(named, (per_dev, per_dev)).T.astype(jnp.int32)[:, :1]
    pick = (named == lax.broadcasted_iota(jnp.int32, (per_dev, pool_rows), 1)).astype(jnp.bfloat16)

    def pick_into(target, places):
        @pl.loop(0, half // tile)
        def _(index):
            columns = pl.ds(pl.multiple_of(index * tile, tile), tile)
            picked = dot(pick, pool_buf[:, columns], NN).astype(jnp.bfloat16)
            for chunk in range(CHUNKS):
                target[places[chunk], columns] = picked[chunk * cut : (chunk + 1) * cut]

    pool_far.wait()
    pick_into(far_x, [pl.ds(chunk * cut, cut) for chunk in range(CHUNKS)])
    pool_own = pltpu.make_async_copy(pool_ref.at[:, half_of(grp)], pool_buf, pool_sem.at[1])
    pool_own.start()
    for chunk in range(CHUNKS):
        piece = pl.ds(chunk * cut, cut)
        if chunk > 0:
            token_copy(0, chunk, ("x", 0, 0), cot_ref.at[piece, half_of(other)]).start()
        token_copy(1, chunk, ("x", 0, 0), far_x.at[piece]).start()
    pool_own.wait()
    pick_into(tok_x, [token_rows(0, 0, chunk) for chunk in range(CHUNKS)])
    for chunk in range(CHUNKS):
        for bit in reversed(range(near_bits)):
            token_copy(1, chunk, (0, 0, bit)).start()
    for copy in local:
        copy.wait()

    exponent = expo_ref[0]
    unscale = jnp.float32(1.0)
    for bit in range(4):
        factor = jnp.where((exponent // 2**bit) % 2 == 1, jnp.float32(0.5 ** (2**bit)), jnp.float32(1.0))
        unscale = unscale * factor

    own_group = row // group_rows

    def group_at(order):
        return (own_group + order) % groups

    def group_span(order):
        return pl.ds(pl.multiple_of(group_at(order) * lanes, lanes), lanes)

    blocks = [(rel, mask) for rel in range(2) for mask in range(0, near, 2)]

    def part_copy(order, rel, mask, part, outgoing=True):
        where = block_rows(rel, mask, part)
        received = (1 - rel if outgoing else rel, mask)
        return remote(
            sent_part.at[order, where],
            got_part.at[order, where],
            send_p.at[order, blocks.index((rel, mask)), part],
            recv_p.at[order, blocks.index(received), part],
            across,
        )

    def block_rows(rel, mask, part=None):
        base = (grp if rel == 0 else other) * near + flipped(mask) - bit_of[0]
        if part is None:
            return pl.ds(pl.multiple_of(base * per_dev, block), block)
        return pl.ds(pl.multiple_of(base * per_dev + part * 2 * cut, 2 * cut), 2 * cut)

    def forward(order, rel, mask, part=None):
        where = block_rows(rel, mask, part)
        hidden = group_span(order)
        pair = weights[0:2, hidden, :].reshape(2 * lanes, half)
        acts = dot(tok_x[where, :], pair, NT)
        down = dot(tok_c[where, :], weights[2, hidden, :], NT)
        own_part[order, where, 0 : 2 * lanes] = acts
        own_part[order, where, 2 * lanes : 3 * lanes] = down
        sent_part[order, where, 0 : 2 * lanes] = acts.astype(jnp.bfloat16)
        sent_part[order, where, 2 * lanes : 3 * lanes] = down.astype(jnp.bfloat16)
        for piece in range(CHUNKS) if part is None else [part]:
            part_copy(order, rel, mask, piece).start()

    def backward_deltas(order, rel, mask, part):
        where = block_rows(rel, mask, part)
        part_copy(order, rel, mask, part, False).wait_recv()
        total = own_part[order, where, :] + got_part[order, where, :].astype(jnp.float32)
        gate_act, up_act = total[:, :lanes], total[:, lanes : 2 * lanes]
        delta_hidden = unscale * total[:, 2 * lanes :]
        sig = jax.nn.sigmoid(gate_act)
        made = (
            delta_hidden * up_act * sig * (1.0 + gate_act * (1.0 - sig)),
            delta_hidden * gate_act * sig,
            gate_act * sig * up_act,
        )
        for kind in range(3):
            deltas[kind * lanes : (kind + 1) * lanes, where] = made[kind].T.astype(jnp.bfloat16)

    def pair_grads(order):
        hidden = group_span(order)

        @pl.loop(0, half // tile)
        def _(index):
            columns = pl.ds(pl.multiple_of(index * tile, tile), tile)
            pair = dot(deltas[: 2 * lanes, :], tok_x[:, columns], NN).astype(jnp.bfloat16)
            grads[0, hidden, columns] = pair[:lanes]
            grads[1, hidden, columns] = pair[lanes:]

    def down_grads(order):
        hidden = group_span(order)

        @pl.loop(0, half // tile)
        def _(index):
            columns = pl.ds(pl.multiple_of(index * tile, tile), tile)
            down = unscale * dot(deltas[2 * lanes :, :], tok_c[:, columns], NN)
            grads[2, hidden, columns] = down.astype(jnp.bfloat16)

    def await_sibling(rel, mask, chunk):
        for array in range(2):
            token_arrival(array, chunk, rel, mask + 1).wait_recv()

    def arrival_order(rel, index):
        if rel == 0:
            return divmod(index, CHUNKS)
        chunk, array = divmod(index, 2)
        return array, chunk

    ready = {(0, 0, part): 0 for part in range(CHUNKS)}
    deferred = groups > 1
    weight_steps = 3 * (last - 1) if deferred else 3 * last
    steps = weight_steps
    for start, rel, mask in relays:
        for index in range(2 * CHUNKS):
            _, part = arrival_order(rel, index)
            ready[(rel, mask, part)] = start + index
        steps = max(steps, start + 2 * CHUNKS - 1)
    split = relays[-1][1:]
    pieces = [key + (part,) for key in blocks for part in range(CHUNKS)]
    own_ready = 3 * (group_rows - 1)
    done_forward, done_deltas = [], []

    def advance(step):
        for key in blocks:
            parts = [
                part
                for part in range(CHUNKS)
                if key + (part,) not in done_forward and ready[key + (part,)] <= step
            ]
            if not parts or (len(parts) < CHUNKS and key != split):
                continue
            for part in parts:
                await_sibling(*key, part)
                done_forward.append(key + (part,))
            if len(parts) == CHUNKS:
                forward(0, *key)
            else:
                for part in parts:
                    forward(0, *key, part)

    for step in range(1, steps + 1):
        if step <= weight_steps:
            hop, kind = divmod(step - 1, 3)
            for direction in range(2):

                @pl.when(weight_arrives(direction, hop))
                def _(direction=direction, hop=hop, kind=kind):
                    weight_arrival(direction, hop, kind).wait_recv()

                if hop + 1 < last:

                    @pl.when(
                        jnp.logical_and(
                            weight_arrives(direction, hop), weight_sends(direction, hop + 1)
                        )
                    )
                    def _(direction=direction, hop=hop, kind=kind):
                        weight_copy(direction, hop + 1, kind).start()

        for start, rel, mask in relays:
            if start <= step < start + 2 * CHUNKS:
                array, chunk = arrival_order(rel, step - start)
                token_arrival(array, chunk, rel, mask).wait_recv()
                for bit in reversed(range(low_bit(mask, near_bits))):
                    token_copy(array, chunk, (rel, mask, bit)).start()
        for rel, mask, part in pieces:
            if (
                (rel, mask, part) in done_forward
                and (1 - rel, mask, part) in done_forward
                and (rel, mask, part) not in done_deltas
            ):
                backward_deltas(0, rel, mask, part)
                done_deltas.append((rel, mask, part))
        if step >= own_ready + 1:
            advance(step)
    advance(steps)
    for rel, mask, part in pieces[::-1]:
        if (rel, mask, part) not in done_deltas:
            backward_deltas(0, rel, mask, part)
    down_grads(0)

    grad_cuts = max(1, units // 32)
    grad_rows = units // grad_cuts

    def grad_place(unit, index):
        kind, part = (index // grad_cuts + 2) % 3, index % grad_cuts
        start = unit * units + part * grad_rows
        return kind, pl.ds(pl.multiple_of(start, grad_rows), grad_rows)

    def pass_on(going_left, unit, index):
        kind, where = grad_place(unit, index)
        landing = from_right if going_left else from_left
        direction = 0 if going_left else 1
        copy = remote(
            grads.at[kind, where],
            landing.at[kind, where],
            send_g.at[direction, unit, index],
            recv_g.at[direction, unit, index],
            left if going_left else right,
        )

        @pl.when(row < last if going_left else row > 0)
        def _():
            copy.wait_recv()
            summed = grads[kind, where, :].astype(jnp.float32) + landing[kind, where, :].astype(
                jnp.float32
            )
            grads[kind, where, :] = summed.astype(jnp.bfloat16)

        copy.start()

    def out_copy(index):
        kind, part = (index // grad_cuts + 2) % 3, index % grad_cuts
        to = pl.ds(pl.multiple_of(part * grad_rows, grad_rows), grad_rows)
        pair = pltpu.make_async_copy(
            out_buf.at[kind, to], pair_out.at[kind % 2, to], out_sem.at[index]
        )
        down = pltpu.make_async_copy(out_buf.at[kind, to], down_out.at[to], out_sem.at[index])
        return kind, to, pair, down

    def finish(index):
        kind, where = grad_place(row, index)
        acc[...] = grads[kind, where, :].astype(jnp.float32)
        for direction, landing, present in ((1, from_left, row > 0), (0, from_right, row < last)):

            @pl.when(present)
            def _(direction=direction, landing=landing):
                place = landing.at[kind, where]
                remote(
                    place,
                    place,
                    send_g.at[direction, row, index],
                    recv_g.at[direction, row, index],
                    across,
                ).wait_recv()
                acc[...] += landing[kind, where, :].astype(jnp.float32)

        _, to, pair, down = out_copy(index)
        out_buf[kind, to, :] = acc[...].astype(jnp.bfloat16)

        @pl.when(kind < 2)
        def _():
            pair.start()

        @pl.when(kind == 2)
        def _():
            down.start()

    upper = row >= rows // 2
    lower = row < rows // 2

    def pass_units(unit, first, end, finishing=False):
        mirror = last - unit

        @pl.loop(first, end + 1)
        def _(index):
            now, later = index < end, index > first

            @pl.when(jnp.logical_and(jnp.logical_and(upper, row > unit), now))
            def _():
                pass_on(True, unit, index)

            @pl.when(jnp.logical_and(jnp.logical_and(lower, row < mirror), now))
            def _():
                pass_on(False, mirror, index)

            @pl.when(jnp.logical_and(jnp.logical_and(upper, row < mirror), later))
            def _():
                pass_on(False, mirror, index - 1)

            @pl.when(jnp.logical_and(jnp.logical_and(lower, row > unit), later))
            def _():
                pass_on(True, unit, index - 1)

            if finishing:

                @pl.when(later)
                def _():
                    finish(index - 1)

    order_left = [last - 1] + list(range(last - 1))
    total = 3 * grad_cuts
    early = group_rows > 1
    held_back = 1 if early and last > 1 else 0
    if early:
        pass_units(order_left[0], 0, grad_cuts, last == 1)
    if deferred:
        for kind in range(3):
            for direction in range(2):

                @pl.when(weight_arrives(direction, last - 1))
                def _(direction=direction, kind=kind):
                    weight_arrival(direction, last - 1, kind).wait_recv()

    ahead = blocks[:2] if deferred else []
    for key in ahead:
        forward(1, *key)
    pair_grads(0)
    if early:
        pass_units(order_left[0], grad_cuts, total - held_back, last == 1)
    for order in range(1, groups):
        for key in blocks:
            if order > 1 or key not in ahead:
                forward(order, *key)
        for key in pieces:
            backward_deltas(order, *key)
        down_grads(order)
        pair_grads(order)
    if not early:
        pass_units(order_left[0], 0, total)
    for unit in order_left[1:]:
        pass_units(unit, 0, total, unit == order_left[-1])
    if held_back:
        pass_units(order_left[0], total - held_back, total)

    for kind in range(3):
        for direction in range(2):
            for hop in range(last):

                @pl.when(weight_sends(direction, hop))
                def _(kind=kind, direction=direction, hop=hop):
                    weight_copy(direction, hop, kind).wait_send()

    for array in range(2):
        for chunk in range(CHUNKS):
            for key in sends:
                token_copy(array, chunk, key).wait_send()
    for order in range(groups):
        for key in pieces:
            part_copy(order, *key).wait_send()

    @pl.loop(0, 3 * grad_cuts)
    def _(index):
        for unit in range(rows):
            kind, where = grad_place(unit, index)
            place = grads.at[kind, where]
            for direction, goes in ((0, row > unit), (1, row < unit)):

                @pl.when(goes)
                def _(direction=direction, unit=unit, place=place):
                    remote(
                        place,
                        place,
                        send_g.at[direction, unit, index],
                        recv_g.at[direction, unit, index],
                        across,
                    ).wait_send()

        kind, _, pair, down = out_copy(index)

        @pl.when(kind < 2)
        def _():
            pair.wait()

        @pl.when(kind == 2)
        def _():
            down.wait()


def settle(pair_ref, down_ref, pair_out, down_out, held, come, go):
    units = down_ref.shape[0]
    rows = units // 2
    moves = []
    for index in range(6):
        kind, where = index // 2, pl.ds(index % 2 * rows, rows)
        source = pair_ref.at[kind, where] if kind < 2 else down_ref.at[where]
        target = pair_out.at[kind, where] if kind < 2 else down_out.at[where]
        moves.append(
            (
                pltpu.make_async_copy(source, held.at[index], come.at[index]),
                pltpu.make_async_copy(held.at[index], target, go.at[index]),
            )
        )
    for arrive, _ in moves:
        arrive.start()
    for arrive, leave in moves:
        arrive.wait()
        leave.start()
    for _, leave in moves:
        leave.wait()


def per_device(rows, near_bits, x_pool, token_ids, cotangent, gate_up, down_weight, loss_exponent):
    near = 2**near_bits
    _, units, half = gate_up.shape
    per_dev = token_ids.shape[0]
    span = rows * units
    group_rows = max(1, min(rows, 128 // units))
    groups, lanes = rows // group_rows, group_rows * units
    token_count = 2 * near * per_dev
    grad_cuts = max(1, units // 32)
    sends, _ = token_plan(near_bits)
    bf16, f32 = jnp.bfloat16, jnp.float32
    anywhere = pl.BlockSpec(memory_space=pl.ANY)
    dma = pltpu.SemaphoreType.DMA
    blocks = near
    out = pl.pallas_call(
        functools.partial(kernel, near_bits, rows),
        out_shape=(
            jax.ShapeDtypeStruct((2, units, half), bf16),
            jax.ShapeDtypeStruct((units, half), bf16),
        ),
        in_specs=[
            pl.BlockSpec(memory_space=pltpu.VMEM),
            pl.BlockSpec(memory_space=pltpu.SMEM),
            anywhere,
            anywhere,
            anywhere,
            anywhere,
        ],
        out_specs=(anywhere, anywhere),
        scratch_shapes=[
            pltpu.VMEM((token_count, half), bf16),
            pltpu.VMEM((token_count, half), bf16),
            pltpu.VMEM((per_dev, half), bf16),
            pltpu.VMEM((x_pool.shape[0], half), bf16),
            pltpu.VMEM((3, span, half), bf16),
            pltpu.VMEM((3, span, half), bf16),
            pltpu.VMEM((3, span, half), bf16),
            pltpu.VMEM((3, span, half), bf16),
            pltpu.VMEM((groups, token_count, 3 * lanes), f32),
            pltpu.VMEM((groups, token_count, 3 * lanes), bf16),
            pltpu.VMEM((groups, token_count, 3 * lanes), bf16),
            pltpu.VMEM((3 * lanes, token_count), bf16),
            pltpu.VMEM((units // grad_cuts, half), f32),
            pltpu.VMEM((3, units, half), bf16),
            dma((2, rows - 1, 3)),
            dma((2, rows - 1, 3)),
            dma((2, CHUNKS, len(sends))),
            dma((2, CHUNKS, 2 * near)),
            dma((groups, blocks, CHUNKS)),
            dma((groups, blocks, CHUNKS)),
            dma((2, rows, 3 * grad_cuts)),
            dma((2, rows, 3 * grad_cuts)),
            dma((3 + CHUNKS,)),
            dma((2,)),
            dma((3 * grad_cuts,)),
        ],
        compiler_params=pltpu.CompilerParams(
            collective_id=0, has_side_effects=True, vmem_limit_bytes=67_000_000
        ),
    )(token_ids.reshape(1, per_dev), loss_exponent, x_pool, cotangent, gate_up, down_weight)
    return pl.pallas_call(
        settle,
        out_shape=(
            jax.ShapeDtypeStruct((2, units, half), bf16),
            jax.ShapeDtypeStruct((units, half), bf16),
        ),
        in_specs=[anywhere, anywhere],
        out_specs=(anywhere, anywhere),
        scratch_shapes=[pltpu.VMEM((6, units // 2, half), bf16), dma((6,)), dma((6,))],
    )(*out)


def solution(mesh):
    rows, near_bits = line_of(mesh.shape["wide"])
    return jax.shard_map(
        functools.partial(per_device, rows, near_bits),
        mesh=mesh,
        in_specs=(
            P(("grp", "wide"), None),
            P(("grp", "wide")),
            P(("grp", "wide"), None),
            P(None, "wide", "grp"),
            P("wide", "grp"),
            P(),
        ),
        out_specs=(P(None, "wide", "grp"), P("wide", "grp")),
        check_vma=False,
    )
```

```python
import functools

import jax
import jax.numpy as jnp
from jax import lax
from jax.experimental import pallas as pl
from jax.experimental.pallas import tpu as pltpu
from jax.sharding import PartitionSpec as P

MESH = pl.DeviceIdType.MESH
NT = (((1,), (1,)), ((), ()))
NN = (((1,), (0,)), ((), ()))
CHUNKS = 2


def line_of(wide_count):
    bits = wide_count.bit_length() - 1
    near_bits = bits - bits // 2
    return wide_count // 2**near_bits, near_bits


def low_bit(mask, bits):
    return (mask & -mask).bit_length() - 1 if mask else bits


def dot(left_side, right_side, dims):
    return lax.dot_general(left_side, right_side, dims, preferred_element_type=jnp.float32)


def token_plan(near_bits):
    near = 2**near_bits
    sends = [("x", 0, 0)]
    for rel in range(2):
        for mask in range(near):
            sends += [(rel, mask, bit) for bit in range(low_bit(mask, near_bits))]
    masks = [mask for mask in range(2, near, 2)]
    masks.sort(key=lambda mask: (bin(mask).count("1"), -mask))
    keyed = [(0, mask) for mask in masks] + [(1, mask) for mask in [0] + masks]
    keyed.sort(key=lambda item: bin(item[1]).count("1") * 2 + (item[0] * 2 if item[1] else 0))
    relays = [(1 + 2 * CHUNKS * (index // 2), rel, mask) for index, (rel, mask) in enumerate(keyed)]
    return sends, relays


def kernel(
    near_bits,
    rows,
    ids_ref,
    expo_ref,
    pool_ref,
    cot_ref,
    gate_up_ref,
    down_ref,
    pair_out,
    down_out,
    tok_x,
    tok_c,
    far_x,
    pool_buf,
    weights,
    grads,
    from_left,
    from_right,
    own_part,
    sent_part,
    got_part,
    deltas,
    acc,
    out_buf,
    send_w,
    recv_w,
    send_t,
    recv_t,
    send_p,
    recv_p,
    send_g,
    recv_g,
    local_sem,
    pool_sem,
    out_sem,
):
    near = 2**near_bits
    wide_count = rows * near
    grp = lax.axis_index("grp")
    wide = lax.axis_index("wide")
    other = 1 - grp
    row = wide // near
    slot = wide % near
    last = rows - 1
    per_dev = ids_ref.shape[1]
    pool_rows = pool_ref.shape[0]
    half = tok_x.shape[1]
    units = gate_up_ref.shape[1]
    span = rows * units
    group_rows = max(1, min(rows, 128 // units))
    groups = rows // group_rows
    lanes = group_rows * units
    cut = per_dev // CHUNKS
    block = 2 * per_dev
    tile = 896

    bit_of = [(slot // 2**bit) % 2 for bit in range(near_bits)]

    def flipped(mask):
        place = slot
        for bit in range(near_bits):
            if mask >> bit & 1:
                place = place + 2**bit * (1 - 2 * bit_of[bit])
        return place

    across = {"grp": other}
    left = {"wide": jnp.maximum(wide - near, 0)}
    right = {"wide": jnp.minimum(wide + near, wide_count - 1)}
    partner = [{"wide": row * near + flipped(2**bit)} for bit in range(near_bits)]

    barrier = pltpu.get_barrier_semaphore()

    def greet(device):
        pl.semaphore_signal(barrier, inc=1, device_id=device, device_id_type=MESH)

    for device in [across] + partner:
        greet(device)

    @pl.when(row > 0)
    def _():
        greet(left)

    @pl.when(row < last)
    def _():
        greet(right)

    neighbours = (row + last) // rows + (2 * last - row) // rows
    pl.semaphore_wait(barrier, 1 + near_bits + neighbours)

    def remote(source, target, sent, received, device):
        return pltpu.make_async_remote_copy(
            src_ref=source,
            dst_ref=target,
            send_sem=sent,
            recv_sem=received,
            device_id=device,
            device_id_type=MESH,
        )

    def unit_rows(origin):
        return pl.ds(pl.multiple_of(origin * units, units), units)

    def weight_copy(direction, hop, kind, source=None):
        going_right = direction == 0
        origin = row - hop if going_right else row + hop
        origin = jnp.clip(origin, 0, last)
        place = weights.at[kind, unit_rows(origin)]
        return remote(
            place if source is None else source,
            place,
            send_w.at[direction, hop, kind],
            recv_w.at[direction, hop, kind],
            right if going_right else left,
        )

    def weight_sends(direction, hop):
        going_right = direction == 0
        held = row >= hop if going_right else row <= last - hop
        open_end = row < last if going_right else row > 0
        return jnp.logical_and(held, open_end)

    def weight_arrives(direction, hop):
        return row >= hop + 1 if direction == 0 else row <= last - hop - 1

    def weight_arrival(direction, hop, kind):
        origin = row - hop - 1 if direction == 0 else row + hop + 1
        place = weights.at[kind, unit_rows(jnp.clip(origin, 0, last))]
        device = left if direction == 0 else right
        return remote(
            place, place, send_w.at[direction, hop, kind], recv_w.at[direction, hop, kind], device
        )

    def weight_source(kind):
        return gate_up_ref.at[kind] if kind < 2 else down_ref

    for kind in range(3):
        for direction in range(2):

            @pl.when(weight_sends(direction, 0))
            def _(kind=kind, direction=direction):
                weight_copy(direction, 0, kind, weight_source(kind)).start()

    sends, relays = token_plan(near_bits)
    send_index = {key: index for index, key in enumerate(sends)}
    buffers = (tok_c, tok_x)

    def token_rows(rel, mask, chunk):
        core = bit_of[0] if mask % 2 == 0 else 1 - bit_of[0]
        base = (grp if rel == 0 else other) * near + flipped(mask) - core
        start = base * per_dev + (2 * chunk + core) * cut
        return pl.ds(pl.multiple_of(start, cut), cut)

    def token_copy(array, chunk, key, source=None):
        rel, mask, bit = key
        if rel == "x":
            place = buffers[array].at[token_rows(0, 0, chunk)]
            device, arrives = across, near
        else:
            place = buffers[array].at[token_rows(rel, mask, chunk)]
            device, arrives = partner[bit], rel * near + mask + 2**bit
        return remote(
            place if source is None else source,
            place,
            send_t.at[array, chunk, send_index[key]],
            recv_t.at[array, chunk, arrives],
            device,
        )

    def token_arrival(array, chunk, rel, mask):
        place = buffers[array].at[token_rows(rel, mask, chunk)]
        device = across if mask == 0 else partner[low_bit(mask, near_bits)]
        return remote(
            place,
            place,
            send_t.at[array, chunk, 0],
            recv_t.at[array, chunk, rel * near + mask],
            device,
        )

    def half_of(which):
        return pl.ds(pl.multiple_of(which * half, half), half)

    pool_far = pltpu.make_async_copy(pool_ref.at[:, half_of(other)], pool_buf, pool_sem.at[0])
    pool_far.start()
    for chunk in range(CHUNKS):
        piece = pl.ds(chunk * cut, cut)
        if chunk == 0:
            token_copy(0, chunk, ("x", 0, 0), cot_ref.at[piece, half_of(other)]).start()
        for bit in reversed(range(near_bits)):
            token_copy(0, chunk, (0, 0, bit), cot_ref.at[piece, half_of(grp)]).start()
    local = [
        pltpu.make_async_copy(
            weight_source(kind), weights.at[kind, unit_rows(row)], local_sem.at[kind]
        )
        for kind in range(3)
    ]
    for chunk in range(CHUNKS):
        piece = pl.ds(chunk * cut, cut)
        local.append(
            pltpu.make_async_copy(
                cot_ref.at[piece, half_of(grp)],
                tok_c.at[token_rows(0, 0, chunk)],
                local_sem.at[3 + chunk],
            )
        )
    for copy in local:
        copy.start()

    first_row = (grp * wide_count + wide) * pool_rows
    named = (ids_ref[...] - first_row).astype(jnp.float32)
    named = jnp.broadcast_to(named, (per_dev, per_dev)).T.astype(jnp.int32)[:, :1]
    pick = (named == lax.broadcasted_iota(jnp.int32, (per_dev, pool_rows), 1)).astype(jnp.bfloat16)

    def pick_into(target, places):
        @pl.loop(0, half // tile)
        def _(index):
            columns = pl.ds(pl.multiple_of(index * tile, tile), tile)
            picked = dot(pick, pool_buf[:, columns], NN).astype(jnp.bfloat16)
            for chunk in range(CHUNKS):
                target[places[chunk], columns] = picked[chunk * cut : (chunk + 1) * cut]

    pool_far.wait()
    pick_into(far_x, [pl.ds(chunk * cut, cut) for chunk in range(CHUNKS)])
    pool_own = pltpu.make_async_copy(pool_ref.at[:, half_of(grp)], pool_buf, pool_sem.at[1])
    pool_own.start()
    for chunk in range(CHUNKS):
        piece = pl.ds(chunk * cut, cut)
        if chunk > 0:
            token_copy(0, chunk, ("x", 0, 0), cot_ref.at[piece, half_of(other)]).start()
        token_copy(1, chunk, ("x", 0, 0), far_x.at[piece]).start()
    pool_own.wait()
    pick_into(tok_x, [token_rows(0, 0, chunk) for chunk in range(CHUNKS)])
    for chunk in range(CHUNKS):
        for bit in reversed(range(near_bits)):
            token_copy(1, chunk, (0, 0, bit)).start()
    for copy in local:
        copy.wait()

    exponent = expo_ref[0]
    unscale = jnp.float32(1.0)
    for bit in range(4):
        factor = jnp.where((exponent // 2**bit) % 2 == 1, jnp.float32(0.5 ** (2**bit)), jnp.float32(1.0))
        unscale = unscale * factor

    own_group = row // group_rows

    def group_at(order):
        return (own_group + order) % groups

    def group_span(order):
        return pl.ds(pl.multiple_of(group_at(order) * lanes, lanes), lanes)

    blocks = [(rel, mask) for rel in range(2) for mask in range(0, near, 2)]

    def part_copy(order, rel, mask, part, outgoing=True):
        where = block_rows(rel, mask, part)
        received = (1 - rel if outgoing else rel, mask)
        return remote(
            sent_part.at[order, where],
            got_part.at[order, where],
            send_p.at[order, blocks.index((rel, mask)), part],
            recv_p.at[order, blocks.index(received), part],
            across,
        )

    def block_rows(rel, mask, part=None):
        base = (grp if rel == 0 else other) * near + flipped(mask) - bit_of[0]
        if part is None:
            return pl.ds(pl.multiple_of(base * per_dev, block), block)
        return pl.ds(pl.multiple_of(base * per_dev + part * 2 * cut, 2 * cut), 2 * cut)

    def forward(order, rel, mask, part=None):
        where = block_rows(rel, mask, part)
        hidden = group_span(order)
        pair = weights[0:2, hidden, :].reshape(2 * lanes, half)
        acts = dot(tok_x[where, :], pair, NT)
        down = dot(tok_c[where, :], weights[2, hidden, :], NT)
        own_part[order, where, 0 : 2 * lanes] = acts
        own_part[order, where, 2 * lanes : 3 * lanes] = down
        sent_part[order, where, 0 : 2 * lanes] = acts.astype(jnp.bfloat16)
        sent_part[order, where, 2 * lanes : 3 * lanes] = down.astype(jnp.bfloat16)
        for piece in range(CHUNKS) if part is None else [part]:
            part_copy(order, rel, mask, piece).start()

    def backward_deltas(order, rel, mask, part):
        where = block_rows(rel, mask, part)
        part_copy(order, rel, mask, part, False).wait_recv()
        total = own_part[order, where, :] + got_part[order, where, :].astype(jnp.float32)
        gate_act, up_act = total[:, :lanes], total[:, lanes : 2 * lanes]
        delta_hidden = unscale * total[:, 2 * lanes :]
        sig = jax.nn.sigmoid(gate_act)
        made = (
            delta_hidden * up_act * sig * (1.0 + gate_act * (1.0 - sig)),
            delta_hidden * gate_act * sig,
            gate_act * sig * up_act,
        )
        for kind in range(3):
            deltas[kind * lanes : (kind + 1) * lanes, where] = made[kind].T.astype(jnp.bfloat16)

    def pair_grads(order):
        hidden = group_span(order)

        @pl.loop(0, half // tile)
        def _(index):
            columns = pl.ds(pl.multiple_of(index * tile, tile), tile)
            pair = dot(deltas[: 2 * lanes, :], tok_x[:, columns], NN).astype(jnp.bfloat16)
            grads[0, hidden, columns] = pair[:lanes]
            grads[1, hidden, columns] = pair[lanes:]

    def down_grads(order):
        hidden = group_span(order)

        @pl.loop(0, half // tile)
        def _(index):
            columns = pl.ds(pl.multiple_of(index * tile, tile), tile)
            down = unscale * dot(deltas[2 * lanes :, :], tok_c[:, columns], NN)
            grads[2, hidden, columns] = down.astype(jnp.bfloat16)

    def await_sibling(rel, mask, chunk):
        for array in range(2):
            token_arrival(array, chunk, rel, mask + 1).wait_recv()

    def arrival_order(rel, index):
        if rel == 0:
            return divmod(index, CHUNKS)
        chunk, array = divmod(index, 2)
        return array, chunk

    ready = {(0, 0, part): 0 for part in range(CHUNKS)}
    deferred = groups > 1
    weight_steps = 3 * (last - 1) if deferred else 3 * last
    steps = weight_steps
    for start, rel, mask in relays:
        for index in range(2 * CHUNKS):
            _, part = arrival_order(rel, index)
            ready[(rel, mask, part)] = start + index
        steps = max(steps, start + 2 * CHUNKS - 1)
    split = relays[-1][1:]
    pieces = [key + (part,) for key in blocks for part in range(CHUNKS)]
    own_ready = 3 * (group_rows - 1)
    done_forward, done_deltas = [], []

    def advance(step):
        for key in blocks:
            parts = [
                part
                for part in range(CHUNKS)
                if key + (part,) not in done_forward and ready[key + (part,)] <= step
            ]
            if not parts or (len(parts) < CHUNKS and key != split):
                continue
            for part in parts:
                await_sibling(*key, part)
                done_forward.append(key + (part,))
            if len(parts) == CHUNKS:
                forward(0, *key)
            else:
                for part in parts:
                    forward(0, *key, part)

    for step in range(1, steps + 1):
        if step <= weight_steps:
            hop, kind = divmod(step - 1, 3)
            for direction in range(2):

                @pl.when(weight_arrives(direction, hop))
                def _(direction=direction, hop=hop, kind=kind):
                    weight_arrival(direction, hop, kind).wait_recv()

                if hop + 1 < last:

                    @pl.when(
                        jnp.logical_and(
                            weight_arrives(direction, hop), weight_sends(direction, hop + 1)
                        )
                    )
                    def _(direction=direction, hop=hop, kind=kind):
                        weight_copy(direction, hop + 1, kind).start()

        for start, rel, mask in relays:
            if start <= step < start + 2 * CHUNKS:
                array, chunk = arrival_order(rel, step - start)
                token_arrival(array, chunk, rel, mask).wait_recv()
                for bit in reversed(range(low_bit(mask, near_bits))):
                    token_copy(array, chunk, (rel, mask, bit)).start()
        for rel, mask, part in pieces:
            if (
                (rel, mask, part) in done_forward
                and (1 - rel, mask, part) in done_forward
                and (rel, mask, part) not in done_deltas
            ):
                backward_deltas(0, rel, mask, part)
                done_deltas.append((rel, mask, part))
        if step >= own_ready + 1:
            advance(step)
    advance(steps)
    for rel, mask, part in pieces[::-1]:
        if (rel, mask, part) not in done_deltas:
            backward_deltas(0, rel, mask, part)
    down_grads(0)

    grad_cuts = max(1, units // 32)
    grad_rows = units // grad_cuts

    def grad_place(unit, index):
        kind, part = (index // grad_cuts + 2) % 3, index % grad_cuts
        start = unit * units + part * grad_rows
        return kind, pl.ds(pl.multiple_of(start, grad_rows), grad_rows)

    def pass_on(going_left, unit, index):
        kind, where = grad_place(unit, index)
        landing = from_right if going_left else from_left
        direction = 0 if going_left else 1
        copy = remote(
            grads.at[kind, where],
            landing.at[kind, where],
            send_g.at[direction, unit, index],
            recv_g.at[direction, unit, index],
            left if going_left else right,
        )

        @pl.when(row < last if going_left else row > 0)
        def _():
            copy.wait_recv()
            summed = grads[kind, where, :].astype(jnp.float32) + landing[kind, where, :].astype(
                jnp.float32
            )
            grads[kind, where, :] = summed.astype(jnp.bfloat16)

        copy.start()

    def out_copy(index):
        kind, part = (index // grad_cuts + 2) % 3, index % grad_cuts
        to = pl.ds(pl.multiple_of(part * grad_rows, grad_rows), grad_rows)
        pair = pltpu.make_async_copy(
            out_buf.at[kind, to], pair_out.at[kind % 2, to], out_sem.at[index]
        )
        down = pltpu.make_async_copy(out_buf.at[kind, to], down_out.at[to], out_sem.at[index])
        return kind, to, pair, down

    def finish(index):
        kind, where = grad_place(row, index)
        acc[...] = grads[kind, where, :].astype(jnp.float32)
        for direction, landing, present in ((1, from_left, row > 0), (0, from_right, row < last)):

            @pl.when(present)
            def _(direction=direction, landing=landing):
                place = landing.at[kind, where]
                remote(
                    place,
                    place,
                    send_g.at[direction, row, index],
                    recv_g.at[direction, row, index],
                    across,
                ).wait_recv()
                acc[...] += landing[kind, where, :].astype(jnp.float32)

        _, to, pair, down = out_copy(index)
        out_buf[kind, to, :] = acc[...].astype(jnp.bfloat16)

        @pl.when(kind < 2)
        def _():
            pair.start()

        @pl.when(kind == 2)
        def _():
            down.start()

    upper = row >= rows // 2
    lower = row < rows // 2

    def pass_units(unit, first, end, finishing=False):
        mirror = last - unit

        @pl.loop(first, end + 1)
        def _(index):
            now, later = index < end, index > first

            @pl.when(jnp.logical_and(jnp.logical_and(upper, row > unit), now))
            def _():
                pass_on(True, unit, index)

            @pl.when(jnp.logical_and(jnp.logical_and(lower, row < mirror), now))
            def _():
                pass_on(False, mirror, index)

            @pl.when(jnp.logical_and(jnp.logical_and(upper, row < mirror), later))
            def _():
                pass_on(False, mirror, index - 1)

            @pl.when(jnp.logical_and(jnp.logical_and(lower, row > unit), later))
            def _():
                pass_on(True, unit, index - 1)

            if finishing:

                @pl.when(later)
                def _():
                    finish(index - 1)

    order_left = [last - 1] + list(range(last - 1))
    total = 3 * grad_cuts
    early = group_rows > 1
    held_back = 1 if early and last > 1 else 0
    if early:
        pass_units(order_left[0], 0, grad_cuts, last == 1)
    if deferred:
        for kind in range(3):
            for direction in range(2):

                @pl.when(weight_arrives(direction, last - 1))
                def _(direction=direction, kind=kind):
                    weight_arrival(direction, last - 1, kind).wait_recv()

    ahead = blocks[:2] if deferred else []
    for key in ahead:
        forward(1, *key)
    pair_grads(0)
    if early:
        pass_units(order_left[0], grad_cuts, total - held_back, last == 1)
    for order in range(1, groups):
        for key in blocks:
            if order > 1 or key not in ahead:
                forward(order, *key)
        for key in pieces:
            backward_deltas(order, *key)
        down_grads(order)
        pair_grads(order)
    if not early:
        pass_units(order_left[0], 0, total)
    for unit in order_left[1:]:
        pass_units(unit, 0, total, unit == order_left[-1])
    if held_back:
        pass_units(order_left[0], total - held_back, total)

    for kind in range(3):
        for direction in range(2):
            for hop in range(last):

                @pl.when(weight_sends(direction, hop))
                def _(kind=kind, direction=direction, hop=hop):
                    weight_copy(direction, hop, kind).wait_send()

    for array in range(2):
        for chunk in range(CHUNKS):
            for key in sends:
                token_copy(array, chunk, key).wait_send()
    for order in range(groups):
        for key in pieces:
            part_copy(order, *key).wait_send()

    @pl.loop(0, 3 * grad_cuts)
    def _(index):
        for unit in range(rows):
            kind, where = grad_place(unit, index)
            place = grads.at[kind, where]
            for direction, goes in ((0, row > unit), (1, row < unit)):

                @pl.when(goes)
                def _(direction=direction, unit=unit, place=place):
                    remote(
                        place,
                        place,
                        send_g.at[direction, unit, index],
                        recv_g.at[direction, unit, index],
                        across,
                    ).wait_send()

        kind, _, pair, down = out_copy(index)

        @pl.when(kind < 2)
        def _():
            pair.wait()

        @pl.when(kind == 2)
        def _():
            down.wait()


def settle(pair_ref, down_ref, pair_out, down_out, held, come, go):
    units = down_ref.shape[0]
    rows = units // 2
    moves = []
    for index in range(6):
        kind, where = index // 2, pl.ds(index % 2 * rows, rows)
        source = pair_ref.at[kind, where] if kind < 2 else down_ref.at[where]
        target = pair_out.at[kind, where] if kind < 2 else down_out.at[where]
        moves.append(
            (
                pltpu.make_async_copy(source, held.at[index], come.at[index]),
                pltpu.make_async_copy(held.at[index], target, go.at[index]),
            )
        )
    for arrive, _ in moves:
        arrive.start()
    for arrive, leave in moves:
        arrive.wait()
        leave.start()
    for _, leave in moves:
        leave.wait()


def per_device(rows, near_bits, x_pool, token_ids, cotangent, gate_up, down_weight, loss_exponent):
    near = 2**near_bits
    _, units, half = gate_up.shape
    per_dev = token_ids.shape[0]
    span = rows * units
    group_rows = max(1, min(rows, 128 // units))
    groups, lanes = rows // group_rows, group_rows * units
    token_count = 2 * near * per_dev
    grad_cuts = max(1, units // 32)
    sends, _ = token_plan(near_bits)
    bf16, f32 = jnp.bfloat16, jnp.float32
    anywhere = pl.BlockSpec(memory_space=pl.ANY)
    dma = pltpu.SemaphoreType.DMA
    blocks = near
    out = pl.pallas_call(
        functools.partial(kernel, near_bits, rows),
        out_shape=(
            jax.ShapeDtypeStruct((2, units, half), bf16),
            jax.ShapeDtypeStruct((units, half), bf16),
        ),
        in_specs=[
            pl.BlockSpec(memory_space=pltpu.VMEM),
            pl.BlockSpec(memory_space=pltpu.SMEM),
            anywhere,
            anywhere,
            anywhere,
            anywhere,
        ],
        out_specs=(anywhere, anywhere),
        scratch_shapes=[
            pltpu.VMEM((token_count, half), bf16),
            pltpu.VMEM((token_count, half), bf16),
            pltpu.VMEM((per_dev, half), bf16),
            pltpu.VMEM((x_pool.shape[0], half), bf16),
            pltpu.VMEM((3, span, half), bf16),
            pltpu.VMEM((3, span, half), bf16),
            pltpu.VMEM((3, span, half), bf16),
            pltpu.VMEM((3, span, half), bf16),
            pltpu.VMEM((groups, token_count, 3 * lanes), f32),
            pltpu.VMEM((groups, token_count, 3 * lanes), bf16),
            pltpu.VMEM((groups, token_count, 3 * lanes), bf16),
            pltpu.VMEM((3 * lanes, token_count), bf16),
            pltpu.VMEM((units // grad_cuts, half), f32),
            pltpu.VMEM((3, units, half), bf16),
            dma((2, rows - 1, 3)),
            dma((2, rows - 1, 3)),
            dma((2, CHUNKS, len(sends))),
            dma((2, CHUNKS, 2 * near)),
            dma((groups, blocks, CHUNKS)),
            dma((groups, blocks, CHUNKS)),
            dma((2, rows, 3 * grad_cuts)),
            dma((2, rows, 3 * grad_cuts)),
            dma((3 + CHUNKS,)),
            dma((2,)),
            dma((3 * grad_cuts,)),
        ],
        compiler_params=pltpu.CompilerParams(
            collective_id=0, has_side_effects=True, vmem_limit_bytes=67_000_000
        ),
    )(token_ids.reshape(1, per_dev), loss_exponent, x_pool, cotangent, gate_up, down_weight)
    return pl.pallas_call(
        settle,
        out_shape=(
            jax.ShapeDtypeStruct((2, units, half), bf16),
            jax.ShapeDtypeStruct((units, half), bf16),
        ),
        in_specs=[anywhere, anywhere],
        out_specs=(anywhere, anywhere),
        scratch_shapes=[pltpu.VMEM((6, units // 2, half), bf16), dma((6,)), dma((6,))],
    )(*out)


def solution(mesh):
    rows, near_bits = line_of(mesh.shape["wide"])
    return jax.shard_map(
        functools.partial(per_device, rows, near_bits),
        mesh=mesh,
        in_specs=(
            P(("grp", "wide"), None),
            P(("grp", "wide")),
            P(("grp", "wide"), None),
            P(None, "wide", "grp"),
            P("wide", "grp"),
            P(),
        ),
        out_specs=(P(None, "wide", "grp"), P("wide", "grp")),
        check_vma=False,
    )
```
